32 devices in a mesh: dp: 2 (over z, core), sp: 16 (over x, y).
Axes of the slice: x: 4, y: 4, z: 1, core: 2. Of those that a mesh axis runs over, the one named last changes fastest.
The devices are a block of a 4x4x8 slice.
Arguments:
- x: bfloat16 [4096, 6144], P(('dp', 'sp')), parts along dimension 0
- gain: bfloat16 [6144], replicated
- wq: bfloat16 [6144, 6144], replicated
- wk: bfloat16 [6144, 512], replicated
- wv: bfloat16 [6144, 512], replicated
- wo: bfloat16 [6144, 6144], replicated
Outputs:
- output: bfloat16 [4096, 6144], P(('dp', 'sp')), parts along dimension 0
There are 2 independent parts. The reference program is written for one: setup_inputs(seed, part) draws one part's arguments, and reference() takes and returns one part's arrays. A program takes and returns all parts, laid end to end along the dimension named above; an argument that names none is the same for every part.
All inputs are finite; a program needn't handle non-finite values.
Results may differ from the reference program's by a relative error of at most 0.012.
Values are sent between devices in bfloat16 or wider.
A program may use at most 768 MiB of HBM per device.

```python
import jax
import jax.numpy as jnp
from jax import lax

ROWS = 2048
D = 6144
HEADS = 48
KV_HEADS = 4
HEAD = 128
THETA = 10000


def setup_inputs(seed: int = 0, part: int = 0) -> dict:
    kx, kn, kq, kk, kv, ko = jax.random.split(jax.random.key(seed), 6)

    def weights(key, rows, columns):
        return jax.random.normal(key, (rows, columns), jnp.float32) * rows**-0.5

    drawn = {
        "x": jax.random.normal(jax.random.fold_in(kx, part), (ROWS, D), jnp.float32),
        "gain": 1 + 0.1 * jax.random.normal(kn, (D,), jnp.float32),
        "wq": 2 * weights(kq, D, HEADS * HEAD),
        "wk": 2 * weights(kk, D, KV_HEADS * HEAD),
        "wv": 4 * weights(kv, D, KV_HEADS * HEAD),
        "wo": weights(ko, HEADS * HEAD, D),
    }
    return {k: v.astype(jnp.bfloat16) for k, v in drawn.items()}


def normed(x, gain):
    wide = x.astype(jnp.float32)
    scale = lax.rsqrt(jnp.mean(wide * wide, -1, keepdims=True) + 1e-6)
    return (wide * scale * gain.astype(jnp.float32)).astype(jnp.bfloat16)


def turned(t, place, theta):
    half = t.shape[-1] // 2
    angle = place.astype(jnp.float32)[:, None] * theta ** (-jnp.arange(half, dtype=jnp.float32) / half)
    cos, sin = jnp.cos(angle)[:, None], jnp.sin(angle)[:, None]
    a, b = t[..., :half].astype(jnp.float32), t[..., half:].astype(jnp.float32)
    return jnp.concatenate([a * cos - b * sin, b * cos + a * sin], -1).astype(jnp.bfloat16)


def matmul(a, w):
    return jnp.dot(a, w, preferred_element_type=jnp.float32).astype(jnp.bfloat16)


def einsum(form, a, b):
    return jnp.einsum(form, a.astype(jnp.float32), b.astype(jnp.float32))


def attention(q, k, v):
    scores = einsum("tgsd,ugd->gstu", q, k) * q.shape[-1] ** -0.5
    token = jnp.arange(q.shape[0])
    scores = jnp.where(token[:, None] >= token, scores, -jnp.inf)
    weights = jax.nn.softmax(scores, -1).astype(jnp.bfloat16)
    return einsum("gstu,ugd->tgsd", weights, v).astype(jnp.bfloat16)


def reference(x, gain, wq, wk, wv, wo):
    a, place = normed(x, gain), jnp.arange(ROWS)
    q = turned(matmul(a, wq).reshape(ROWS, HEADS, HEAD), place, THETA).reshape(ROWS, KV_HEADS, -1, HEAD)
    k = turned(matmul(a, wk).reshape(ROWS, KV_HEADS, HEAD), place, THETA)
    v = matmul(a, wv).reshape(ROWS, KV_HEADS, HEAD)
    seen = attention(q, k, v).reshape(ROWS, HEADS * HEAD)
    return (x.astype(jnp.float32) + jnp.dot(seen, wo, preferred_element_type=jnp.float32)).astype(jnp.bfloat16)
```

```python
import functools
import math

import jax
import jax.numpy as jnp
from jax import lax
from jax.experimental import pallas as pl
from jax.experimental.pallas import tpu as pltpu
from jax.sharding import PartitionSpec as P

HEAD = 128
THETA = 10000
GROUP = 12
NEG = -1e30
HIDDEN = 2 * NEG
LOG2E = 1.4426950408889634
CHUNK = 256
STRIP = 512
MESH = pl.DeviceIdType.MESH
VMEM_LIMIT = 67043328


def _dot(a, b):
    return jnp.dot(a, b, preferred_element_type=jnp.float32)


def _kernel(side, slots, x_ref, gain_ref, cos_ref, sin_ref, wq_ref, wk_ref, wv_ref, wo_ref, y_ref,
            xbuf, abuf, wbuf, kv, qt, seen, mix, top, acc,
            wsem, xsem, xsend, xrecv, p1send, p1recv, p2send, p2recv, ssend, srecv, ysem, ysend, yrecv):
    own, depth = x_ref.shape
    half = wq_ref.shape[1] // 2
    heads = half // HEAD
    kvh = heads // GROUP
    nq, no = half // CHUNK, half // CHUNK
    dp, sp = lax.axis_index("dp"), lax.axis_index("sp")
    c = lax.rem(dp, 2)
    other = 1 - c
    partner = dp + 1 - 2 * c
    px, py = lax.div(sp, side), lax.rem(sp, side)

    def device(x, y):
        return {"sp": lax.rem(x + side, side) * side + lax.rem(y + side, side)}

    first = (py, px)
    second = (px, py)
    hop1 = ((device(px, py + 1), device(px, py - 1)), (device(px + 1, py), device(px - 1, py)))
    hop2 = (hop1[1], hop1[0])
    at = lambda p, d: lax.rem(p + d + side, side)

    def columns(ref, n):
        return ref.at[:, pl.ds(pl.multiple_of(n * CHUNK, CHUNK), CHUNK)]

    def chunk(ref, n, slot):
        return pltpu.make_async_copy(columns(ref, n), wbuf.at[slot], wsem.at[slot])

    def q_chunk(j):
        return chunk(wq_ref, c * nq + j, lax.rem(j + 2, slots))

    def o_chunk(j):
        return chunk(wo_ref, c * no + j, lax.rem(j + 2 + nq, slots))

    load_x = pltpu.make_async_copy(x_ref, xbuf.at[c], xsem)
    load_x.start()
    k_chunk, v_chunk = chunk(wk_ref, c, 0), chunk(wv_ref, c, 1)
    k_chunk.start()
    v_chunk.start()
    for j in range(slots - 2):
        q_chunk(j).start()

    barrier = pltpu.get_barrier_semaphore()
    peers = [{"dp": partner}, *hop1[0], *hop1[1]]
    for peer in peers:
        pl.semaphore_signal(barrier, inc=1, device_id=peer, device_id_type=MESH)
    pl.semaphore_wait(barrier, len(peers))

    def remote(src, dst, send, recv, peer):
        return pltpu.make_async_remote_copy(src_ref=src, dst_ref=dst, send_sem=send, recv_sem=recv, device_id=peer, device_id_type=MESH)

    send_x = remote(x_ref, xbuf.at[c], xsend, xrecv, {"dp": partner})
    send_x.start()

    rows = 16

    def norm(s):
        def body(r, _):
            here = pl.ds(pl.multiple_of(r * rows, rows), rows)
            wide = xbuf[s, here, :].astype(jnp.float32)
            scale = lax.rsqrt(jnp.mean(wide * wide, -1, keepdims=True) + 1e-6)
            abuf[s, here, :] = (wide * scale * gain_ref[...].astype(jnp.float32)).astype(jnp.bfloat16)

        lax.fori_loop(0, own // rows, body, None)

    load_x.wait()
    norm(c)
    send_x.wait_recv()
    norm(other)

    def project(slot):
        return _dot(abuf[...].reshape(2 * own, depth), wbuf[slot]).astype(jnp.bfloat16)

    def turned(t):
        t = t.astype(jnp.float32)
        return (t * cos_ref[...] + pltpu.roll(t, HEAD // 2, 1) * sin_ref[...]).astype(jnp.bfloat16)

    def blocks(t):
        return [(s, i, t[s * own : (s + 1) * own, i * HEAD : (i + 1) * HEAD]) for s in range(2) for i in range(CHUNK // HEAD)]

    k_chunk.wait()
    for s, i, t in blocks(project(0)):
        kv[s, second[s], first[s], i, 0] = turned(t)
    v_chunk.wait()
    for s, i, t in blocks(project(1)):
        kv[s, second[s], first[s], i, 1] = t.T

    def piece(s, g, f, h=None):
        ref = kv.at[s, at(second[s], g), at(first[s], f)]
        return ref if h is None else ref.at[h]

    def send(stage, s, n, peer, ref):
        sends, recvs = (p1send, p1recv) if stage == 1 else (p2send, p2recv)
        return remote(ref, ref, sends.at[(s, *n)], recvs.at[(s, *n)], peer)

    def hop1_copy(s, n):
        if n < 2:
            return send(1, s, (n,), hop1[s][n], piece(s, 0, 0))
        return send(1, s, (n,), hop1[s][n - 2], piece(s, 0, -1 if n == 2 else 1, n - 2))

    def hop1_arrival(s, n):
        ref = piece(s, 0, -1 if n == 0 else 1) if n < 2 else piece(s, 0, 2, n - 2)
        return send(1, s, (n,), hop1[s][n % 2], ref)

    order = (0, -1, 1, 2)

    def hop2_copy(s, n, o):
        if n < 2:
            return send(2, s, (n, o), hop2[s][n], piece(s, 0, order[o]))
        return send(2, s, (n, o), hop2[s][n - 2], piece(s, -1 if n == 2 else 1, order[o], n - 2))

    def hop2_arrival(s, n, o):
        ref = piece(s, -1 if n == 0 else 1, order[o]) if n < 2 else piece(s, 2, order[o], n - 2)
        return send(2, s, (n, o), hop2[s][n % 2], ref)

    both = (0, 1)
    for s in both:
        for n in (0, 1):
            hop1_copy(s, n).start()
    for s in both:
        for n in (0, 1):
            hop2_copy(s, n, 0).start()

    def comm1():
        for s in both:
            for n in (0, 1):
                hop1_arrival(s, n).wait_recv()
                hop1_copy(s, n + 2).start()
        for s in both:
            for o in (1, 2):
                for n in (0, 1):
                    hop2_copy(s, n, o).start()

    def comm2():
        for s in both:
            for n in (2, 3):
                hop1_arrival(s, n).wait_recv()
            for n in (0, 1):
                hop2_copy(s, n, 3).start()
        forward(0)

    def forward(o):
        for s in both:
            for n in (0, 1):
                hop2_arrival(s, n, o).wait_recv()
                hop2_copy(s, n + 2, o).start()

    for j in (slots - 2, slots - 1):
        if j < nq:
            q_chunk(j).start()

    def q_step(i, _):
        for e in (0, 1):
            j = 2 * i + e
            q_chunk(j).wait()
            for s, n, t in blocks(project(lax.rem(j + 2, slots))):
                qt[s, j * (CHUNK // HEAD) + n] = turned(t).T

        for e in (0, 1):
            o_chunk(2 * i + e).start()

        @pl.when(i == 2)
        def _():
            comm1()

    lax.fori_loop(0, nq // 2, q_step, None)
    comm2()

    e = HEAD**-0.5 * LOG2E
    cols = GROUP * own
    begin = sp * own
    for s in both:
        for h in range(kvh):
            top[s * kvh + h] = jnp.full((1, cols), NEG, jnp.float32)
            mix[s * kvh + h] = jnp.zeros((HEAD + 8, cols), jnp.float32)

    def unit(s, g, masked):
        keys = side * own
        row = lax.broadcasted_iota(jnp.int32, (keys, STRIP), 0)
        query = lax.rem(lax.broadcasted_iota(jnp.int32, (keys, STRIP), 1), own)
        if masked:
            if s == 0:
                ok = query - row >= g * keys - begin
            else:
                ok = query - (lax.div(row, own) * (side * own) + lax.rem(row, own)) >= g * own - begin
        ones = jnp.ones((8, keys), jnp.bfloat16)
        pieces = [(h, a) for h in range(kvh) for a in range(0, cols, STRIP)]
        per = STRIP // own
        scores = []
        for h, a in pieces:
            k = jnp.concatenate([kv[s, g, f, h, 0] for f in range(side)], axis=0)
            q = jnp.concatenate([qt[s, h * GROUP + a // own + n] for n in range(per)], axis=1)
            scores.append(_dot(k, q))
        weights, keeps = [], []
        for (h, a), sc in zip(pieces, scores):
            if masked:
                sc = jnp.where(ok, sc, HIDDEN)
            old = top[s * kvh + h, :, a : a + STRIP]
            new = jnp.maximum(old, sc.max(axis=0, keepdims=True))
            top[s * kvh + h, :, a : a + STRIP] = new
            weights.append(jnp.exp2((sc - new) * e).astype(jnp.bfloat16))
            keeps.append(jnp.exp2((old - new) * e))
        for (h, a), p, keep in zip(pieces, weights, keeps):
            values = jnp.concatenate([jnp.concatenate([kv[s, g, f, h, 1] for f in range(side)], axis=1), ones], axis=0)
            mix[s * kvh + h, :, a : a + STRIP] = mix[s * kvh + h, :, a : a + STRIP] * keep + _dot(values, p)

    def attend(d):
        for s in both:
            g = at(second[s], d)
            if s == 0:
                some, whole = g <= px, g < px
            else:
                some = g * own <= begin
                whole = (side - 1) * side * own + g * own < begin

            @pl.when(whole)
            def _():
                unit(s, g, False)

            @pl.when(some & jnp.logical_not(whole))
            def _():
                unit(s, g, True)

    attend(0)
    forward(1)
    forward(2)
    forward(3)
    attend(-1)
    attend(1)
    for s in both:
        for n in (2, 3):
            for o in range(side):
                hop2_arrival(s, n, o).wait_recv()
    attend(2)

    def seen_copy(s, h):
        ref = seen.at[c, s, :, pl.ds(h * cols, cols)]
        return remote(ref, ref, ssend.at[s, h], srecv.at[s, h], {"dp": partner})

    for s in both:
        for h in range(kvh):
            m = mix[s * kvh + h]
            out = m[:HEAD] * (1 / m[HEAD : HEAD + 1])
            for n in range(GROUP):
                seen[c, s, :, (h * GROUP + n) * HEAD : (h * GROUP + n + 1) * HEAD] = out[:, n * own : (n + 1) * own].T.astype(jnp.bfloat16)
            seen_copy(s, h).start()

    def o_part(which, j):
        w = wbuf[lax.rem(j + 2 + nq, slots), pl.ds(pl.multiple_of(which * half, half), half), :]
        return _dot(seen[which].reshape(2 * own, half), w)

    def o_step1(i, _):
        for b in (0, 1):
            j = 2 * i + b
            o_chunk(j).wait()
            acc[j] = o_part(c, j)

    lax.fori_loop(0, no // 2, o_step1, None)
    for s in both:
        for h in range(kvh):
            ref = seen.at[other, s, :, pl.ds(h * cols, cols)]
            remote(ref, ref, ssend.at[s, h], srecv.at[s, h], {"dp": partner}).wait_recv()

    def y_copies(j):
        where = y_ref.at[:, pl.ds(pl.multiple_of(c * half + j * CHUNK, CHUNK), CHUNK)]
        there = y_ref.at[:, pl.ds(pl.multiple_of(other * half + j * CHUNK, CHUNK), CHUNK)]
        cut = pl.ds(pl.multiple_of(c * half + j * CHUNK, CHUNK), CHUNK)
        return (pltpu.make_async_copy(xbuf.at[c, :, cut], where, ysem.at[j]),
                remote(xbuf.at[other, :, cut], where, ysend.at[j], yrecv.at[j], {"dp": partner}),
                remote(xbuf.at[other, :, cut], there, ysend.at[j], yrecv.at[j], {"dp": partner}))

    def o_step2(i, _):
        for b in (0, 1):
            j = 2 * i + b
            cut = pl.ds(pl.multiple_of(c * half + j * CHUNK, CHUNK), CHUNK)
            y = (acc[j] + o_part(other, j)) + xbuf[:, :, cut].reshape(2 * own, CHUNK).astype(jnp.float32)
            xbuf[:, :, cut] = y.astype(jnp.bfloat16).reshape(2, own, CHUNK)
            mine, theirs, _ = y_copies(j)
            mine.start()
            theirs.start()

    lax.fori_loop(0, no // 2, o_step2, None)

    for j in range(no):
        mine, theirs, coming = y_copies(j)
        mine.wait()
        theirs.wait_send()
        coming.wait_recv()
    send_x.wait_send()
    for s in both:
        for h in range(kvh):
            seen_copy(s, h).wait_send()
        for n in range(4):
            hop1_copy(s, n).wait_send()
            for o in range(side):
                hop2_copy(s, n, o).wait_send()


def solution(mesh):
    side = math.isqrt(mesh.shape["sp"])

    def step(x, gain, wq, wk, wv, wo):
        own, depth = x.shape
        half = wq.shape[1] // 2
        heads, kvh = half // HEAD, half // HEAD // GROUP
        nq = half // CHUNK
        slots = nq
        cols = GROUP * own
        place = (lax.axis_index("sp") * own + jnp.arange(own)).astype(jnp.float32)
        angle = place[:, None] * THETA ** (-jnp.arange(HEAD // 2, dtype=jnp.float32) / (HEAD // 2))
        cos, sin = jnp.cos(angle), jnp.sin(angle)
        cos, sin = jnp.concatenate([cos, cos], -1), jnp.concatenate([-sin, sin], -1)
        bf, f32, dma = jnp.bfloat16, jnp.float32, pltpu.SemaphoreType.DMA
        vmem, hbm = pl.BlockSpec(memory_space=pltpu.VMEM), pl.BlockSpec(memory_space=pl.ANY)
        return pl.pallas_call(
            functools.partial(_kernel, side, slots),
            out_shape=jax.ShapeDtypeStruct((own, depth), bf),
            in_specs=[hbm, vmem, vmem, vmem, hbm, hbm, hbm, hbm],
            out_specs=hbm,
            scratch_shapes=[
                pltpu.VMEM((2, own, depth), bf),
                pltpu.VMEM((2, own, depth), bf),
                pltpu.VMEM((slots, depth, CHUNK), bf),
                pltpu.VMEM((2, side, side, kvh, 2, own, HEAD), bf),
                pltpu.VMEM((2, heads, HEAD, own), bf),
                pltpu.VMEM((2, 2, own, half), bf),
                pltpu.VMEM((2 * kvh, HEAD + 8, cols), f32),
                pltpu.VMEM((2 * kvh, 1, cols), f32),
                pltpu.VMEM((nq, 2 * own, CHUNK), f32),
                dma((slots,)), dma, dma, dma,
                dma((2, 4)), dma((2, 4)), dma((2, 4, side)), dma((2, 4, side)),
                dma((2, kvh)), dma((2, kvh)),
                dma((nq,)), dma((nq,)), dma((nq,)),
            ],
            compiler_params=pltpu.CompilerParams(collective_id=0, has_side_effects=True, vmem_limit_bytes=VMEM_LIMIT),
        )(x, gain[None], cos, sin, wq, wk, wv, wo)

    tokens, whole = P(("dp", "sp"), None), P(None, None)
    return jax.shard_map(
        step,
        mesh=mesh,
        in_specs=(tokens, P(None), whole, whole, whole, whole),
        out_specs=tokens,
        check_vma=False,
    )
```

```python
import functools
import math

import jax
import jax.numpy as jnp
from jax import lax
from jax.experimental import pallas as pl
from jax.experimental.pallas import tpu as pltpu
from jax.sharding import PartitionSpec as P

HEAD = 128
THETA = 10000
GROUP = 12
NEG = -1e30
HIDDEN = 2 * NEG
LOG2E = 1.4426950408889634
WIDE = 4
STRIP = 512
MESH = pl.DeviceIdType.MESH
VMEM_LIMIT = 67043328


def _dot(a, b):
    return jnp.dot(a, b, preferred_element_type=jnp.float32)


def _kernel(side, groups, x_ref, gain_ref, cos_ref, sin_ref, wq_ref, wk_ref, wv_ref, wo_ref, y_ref,
            xbuf, abuf, wbuf, kv, qt, seen, mix, top, acc,
            wsem, xsem, xsend, xrecv, p1send, p1recv, p2send, p2recv, ssend, srecv, ysem, ysend, yrecv):
    own, depth = x_ref.shape
    tiles = depth // HEAD
    half = wq_ref.shape[1] // 2
    heads = half // HEAD
    kvh = heads // GROUP
    step = WIDE * HEAD
    steps = half // step
    dp, sp = lax.axis_index("dp"), lax.axis_index("sp")
    c = lax.rem(dp, 2)
    other = 1 - c
    partner = {"dp": dp + 1 - 2 * c}
    px, py = lax.div(sp, side), lax.rem(sp, side)

    def device(x, y):
        return {"sp": lax.rem(x + side, side) * side + lax.rem(y + side, side)}

    first = (py, px)
    second = (px, py)
    hop1 = ((device(px, py + 1), device(px, py - 1)), (device(px + 1, py), device(px - 1, py)))
    hop2 = (hop1[1], hop1[0])
    at = lambda p, d: lax.rem(p + d + side, side)

    def tile(ref, n, g, e):
        src = ref.at[:, pl.ds(pl.multiple_of(n * HEAD, HEAD), HEAD)]
        return pltpu.make_async_copy(src, wbuf.at[g, e], wsem.at[g, e])

    def kv_group():
        return [tile(wk_ref if e < kvh else wv_ref, c * kvh + e % kvh, 0, e) for e in range(WIDE)]

    def q_group(i):
        return [tile(wq_ref, c * heads + i * WIDE + e, lax.rem(i + 1, groups), e) for e in range(WIDE)]

    def o_group(i):
        return [tile(wo_ref, c * heads + i * WIDE + e, lax.rem(i + 1 + steps, groups), e) for e in range(WIDE)]

    def start(copies):
        for copy in copies:
            copy.start()

    def wait(copies):
        for copy in copies:
            copy.wait()

    load_x = pltpu.make_async_copy(x_ref, xbuf.at[c], xsem)
    load_x.start()
    start(kv_group())

    barrier = pltpu.get_barrier_semaphore()
    peers = [partner, *hop1[0], *hop1[1]]
    for peer in peers:
        pl.semaphore_signal(barrier, inc=1, device_id=peer, device_id_type=MESH)
    pl.semaphore_wait(barrier, len(peers))

    def remote(src, dst, send, recv, peer):
        return pltpu.make_async_remote_copy(src_ref=src, dst_ref=dst, send_sem=send, recv_sem=recv, device_id=peer, device_id_type=MESH)

    send_x = remote(x_ref, xbuf.at[c], xsend, xrecv, partner)
    send_x.start()
    for i in range(groups - 1):
        start(q_group(i))

    rows = 16

    def norm(s):
        def body(r, _):
            here = pl.ds(pl.multiple_of(r * rows, rows), rows)
            total = jnp.zeros((rows, HEAD), jnp.float32)
            for t in range(tiles):
                wide = xbuf[s, here, t * HEAD : (t + 1) * HEAD].astype(jnp.float32)
                total += wide * wide
            scale = lax.rsqrt(jnp.sum(total, -1, keepdims=True) / depth + 1e-6)
            place = pl.ds(pl.multiple_of(s * own + r * rows, rows), rows)
            for t in range(tiles):
                cut = slice(t * HEAD, (t + 1) * HEAD)
                wide = xbuf[s, here, cut].astype(jnp.float32)
                abuf[t, place, :] = (wide * scale * gain_ref[:, cut].astype(jnp.float32)).astype(jnp.bfloat16)

        lax.fori_loop(0, own // rows, body, None)

    load_x.wait()
    norm(c)
    send_x.wait_recv()
    norm(other)

    def project(g):
        lhs = jnp.concatenate([abuf[t] for t in range(tiles)], axis=1)
        rhs = jnp.concatenate([wbuf[g, e] for e in range(WIDE)], axis=1)
        t = _dot(lhs, rhs).astype(jnp.bfloat16)
        return [(s, e, t[s * own : (s + 1) * own, e * HEAD : (e + 1) * HEAD]) for s in range(2) for e in range(WIDE)]

    def turned(t):
        t = t.astype(jnp.float32)
        return (t * cos_ref[...] + pltpu.roll(t, HEAD // 2, 1) * sin_ref[...]).astype(jnp.bfloat16)

    wait(kv_group())
    for s, e, t in project(0):
        if e < kvh:
            kv[s, second[s], first[s], e, 0] = turned(t)
        else:
            kv[s, second[s], first[s], e - kvh, 1] = t.T

    def piece(s, g, f, h=None):
        ref = kv.at[s, at(second[s], g), at(first[s], f)]
        return ref if h is None else ref.at[h]

    def send(stage, s, n, peer, ref):
        sends, recvs = (p1send, p1recv) if stage == 1 else (p2send, p2recv)
        return remote(ref, ref, sends.at[(s, *n)], recvs.at[(s, *n)], peer)

    def hop1_copy(s, n):
        if n < 2:
            return send(1, s, (n,), hop1[s][n], piece(s, 0, 0))
        return send(1, s, (n,), hop1[s][n - 2], piece(s, 0, -1 if n == 2 else 1, n - 2))

    def hop1_arrival(s, n):
        ref = piece(s, 0, -1 if n == 0 else 1) if n < 2 else piece(s, 0, 2, n - 2)
        return send(1, s, (n,), hop1[s][n % 2], ref)

    order = (0, -1, 1, 2)

    def hop2_copy(s, n, o):
        if n < 2:
            return send(2, s, (n, o), hop2[s][n], piece(s, 0, order[o]))
        return send(2, s, (n, o), hop2[s][n - 2], piece(s, -1 if n == 2 else 1, order[o], n - 2))

    def hop2_arrival(s, n, o):
        ref = piece(s, -1 if n == 0 else 1, order[o]) if n < 2 else piece(s, 2, order[o], n - 2)
        return send(2, s, (n, o), hop2[s][n % 2], ref)

    both = (0, 1)
    for s in both:
        for n in (0, 1):
            hop1_copy(s, n).start()
    for s in both:
        for n in (0, 1):
            hop2_copy(s, n, 0).start()

    def comm1():
        for s in both:
            for n in (0, 1):
                hop1_arrival(s, n).wait_recv()
                hop1_copy(s, n + 2).start()
        for s in both:
            for o in (1, 2):
                for n in (0, 1):
                    hop2_copy(s, n, o).start()

    def comm2():
        for s in both:
            for n in (2, 3):
                hop1_arrival(s, n).wait_recv()
            for n in (0, 1):
                hop2_copy(s, n, 3).start()
        forward(0)

    def forward(o):
        for s in both:
            for n in (0, 1):
                hop2_arrival(s, n, o).wait_recv()
                hop2_copy(s, n + 2, o).start()

    start(q_group(groups - 1))

    def q_step(i, _):
        wait(q_group(i))
        for s, e, t in project(lax.rem(i + 1, groups)):
            qt[s, i * WIDE + e] = turned(t).T
        start(o_group(i))

        @pl.when(i == 2)
        def _():
            comm1()

    lax.fori_loop(0, steps, q_step, None)
    comm2()

    e = HEAD**-0.5 * LOG2E
    cols = GROUP * own
    begin = sp * own
    for s in both:
        for h in range(kvh):
            top[s * kvh + h] = jnp.full((1, cols), NEG, jnp.float32)
            mix[s * kvh + h] = jnp.zeros((HEAD + 8, cols), jnp.float32)

    def unit(s, g, masked):
        keys = side * own
        row = lax.broadcasted_iota(jnp.int32, (keys, STRIP), 0)
        query = lax.rem(lax.broadcasted_iota(jnp.int32, (keys, STRIP), 1), own)
        if masked:
            if s == 0:
                ok = query - row >= g * keys - begin
            else:
                ok = query - (lax.div(row, own) * (side * own) + lax.rem(row, own)) >= g * own - begin
        ones = jnp.ones((8, keys), jnp.bfloat16)
        pieces = [(h, a) for h in range(kvh) for a in range(0, cols, STRIP)]
        per = STRIP // own
        scores = []
        for h, a in pieces:
            k = jnp.concatenate([kv[s, g, f, h, 0] for f in range(side)], axis=0)
            q = jnp.concatenate([qt[s, h * GROUP + a // own + n] for n in range(per)], axis=1)
            scores.append(_dot(k, q))
        weights, keeps = [], []
        for (h, a), sc in zip(pieces, scores):
            if masked:
                sc = jnp.where(ok, sc, HIDDEN)
            old = top[s * kvh + h, :, a : a + STRIP]
            new = jnp.maximum(old, sc.max(axis=0, keepdims=True))
            top[s * kvh + h, :, a : a + STRIP] = new
            weights.append(jnp.exp2((sc - new) * e).astype(jnp.bfloat16))
            keeps.append(jnp.exp2((old - new) * e))
        for (h, a), p, keep in zip(pieces, weights, keeps):
            values = jnp.concatenate([jnp.concatenate([kv[s, g, f, h, 1] for f in range(side)], axis=1), ones], axis=0)
            mix[s * kvh + h, :, a : a + STRIP] = mix[s * kvh + h, :, a : a + STRIP] * keep + _dot(values, p)

    def attend(t, _):
        @pl.when(t == 1)
        def _():
            forward(1)
            forward(2)
            forward(3)

        @pl.when(t == 3)
        def _():
            for s in both:
                for n in (2, 3):
                    for o in range(side):
                        hop2_arrival(s, n, o).wait_recv()

        d = (lax.rem(t + 1, 3) + 1) * lax.div(t + 3, 4)
        for s in both:
            g = at(second[s], d)
            if s == 0:
                some, whole = g <= px, g < px
            else:
                some = g * own <= begin
                whole = (side - 1) * side * own + g * own < begin

            @pl.when(whole)
            def _():
                unit(s, g, False)

            @pl.when(some & jnp.logical_not(whole))
            def _():
                unit(s, g, True)

    lax.fori_loop(0, side, attend, None)

    def seen_part(which, s, h):
        return seen.at[which, pl.ds(h * GROUP, GROUP), pl.ds(s * own, own)]

    def seen_copy(which, s, h):
        return remote(seen_part(which, s, h), seen_part(which, s, h), ssend.at[s, h], srecv.at[s, h], partner)

    for s in both:
        for h in range(kvh):
            over = 1 / mix[s * kvh + h, HEAD : HEAD + 1, :]
            for n in range(GROUP):
                cut = slice(n * own, (n + 1) * own)
                out = mix[s * kvh + h, :HEAD, cut] * over[:, cut]
                seen[c, h * GROUP + n, s * own : (s + 1) * own] = out.T.astype(jnp.bfloat16)
            seen_copy(c, s, h).start()

    def o_part(which, i):
        g = lax.rem(i + 1 + steps, groups)
        there = pl.ds(pl.multiple_of(which * half, half), half)
        lhs = jnp.concatenate([seen[which, t] for t in range(heads)], axis=1)
        rhs = jnp.concatenate([wbuf[g, e, there, :] for e in range(WIDE)], axis=1)
        return _dot(lhs, rhs)

    def o_step1(i, _):
        wait(o_group(i))
        acc[i] = o_part(c, i)

    lax.fori_loop(0, steps, o_step1, None)
    for s in both:
        for h in range(kvh):
            seen_copy(other, s, h).wait_recv()

    def y_copies(i):
        cut = pl.ds(pl.multiple_of(c * half + i * step, step), step)
        coming = pl.ds(pl.multiple_of(other * half + i * step, step), step)
        return (pltpu.make_async_copy(xbuf.at[c, :, cut], y_ref.at[:, cut], ysem.at[i]),
                lambda: remote(xbuf.at[other, :, cut], y_ref.at[:, cut], ysend.at[i], yrecv.at[i], partner),
                lambda: remote(xbuf.at[other, :, cut], y_ref.at[:, coming], ysend.at[i], yrecv.at[i], partner))

    def o_step2(i, _):
        cut = pl.ds(pl.multiple_of(c * half + i * step, step), step)
        y = (acc[i] + o_part(other, i)) + xbuf[:, :, cut].reshape(2 * own, step).astype(jnp.float32)
        xbuf[:, :, cut] = y.astype(jnp.bfloat16).reshape(2, own, step)
        mine, theirs, _ = y_copies(i)
        mine.start()
        theirs().start()

    lax.fori_loop(0, steps, o_step2, None)

    for i in range(steps):
        mine, theirs, coming = y_copies(i)
        mine.wait()
        theirs().wait_send()
        coming().wait_recv()
    send_x.wait_send()
    for s in both:
        for h in range(kvh):
            seen_copy(c, s, h).wait_send()
        for n in range(4):
            hop1_copy(s, n).wait_send()
            for o in range(side):
                hop2_copy(s, n, o).wait_send()


def solution(mesh):
    side = math.isqrt(mesh.shape["sp"])

    def step(x, gain, wq, wk, wv, wo):
        own, depth = x.shape
        half = wq.shape[1] // 2
        heads, kvh = half // HEAD, half // HEAD // GROUP
        steps = half // (WIDE * HEAD)
        groups = steps
        cols = GROUP * own
        place = (lax.axis_index("sp") * own + jnp.arange(own)).astype(jnp.float32)
        angle = place[:, None] * THETA ** (-jnp.arange(HEAD // 2, dtype=jnp.float32) / (HEAD // 2))
        cos, sin = jnp.cos(angle), jnp.sin(angle)
        cos, sin = jnp.concatenate([cos, cos], -1), jnp.concatenate([-sin, sin], -1)
        bf, f32, dma = jnp.bfloat16, jnp.float32, pltpu.SemaphoreType.DMA
        vmem, hbm = pl.BlockSpec(memory_space=pltpu.VMEM), pl.BlockSpec(memory_space=pl.ANY)
        return pl.pallas_call(
            functools.partial(_kernel, side, groups),
            out_shape=jax.ShapeDtypeStruct((own, depth), bf),
            in_specs=[hbm, vmem, vmem, vmem, hbm, hbm, hbm, hbm],
            out_specs=hbm,
            scratch_shapes=[
                pltpu.VMEM((2, own, depth), bf),
                pltpu.VMEM((depth // HEAD, 2 * own, HEAD), bf),
                pltpu.VMEM((groups, WIDE, depth, HEAD), bf),
                pltpu.VMEM((2, side, side, kvh, 2, own, HEAD), bf),
                pltpu.VMEM((2, heads, HEAD, own), bf),
                pltpu.VMEM((2, heads, 2 * own, HEAD), bf),
                pltpu.VMEM((2 * kvh, HEAD + 8, cols), f32),
                pltpu.VMEM((2 * kvh, 1, cols), f32),
                pltpu.VMEM((steps, 2 * own, WIDE * HEAD), f32),
                dma((groups, WIDE)), dma, dma, dma,
                dma((2, 4)), dma((2, 4)), dma((2, 4, side)), dma((2, 4, side)),
                dma((2, kvh)), dma((2, kvh)),
                dma((steps,)), dma((steps,)), dma((steps,)),
            ],
            compiler_params=pltpu.CompilerParams(collective_id=0, has_side_effects=True, vmem_limit_bytes=VMEM_LIMIT),
        )(x, gain[None], cos, sin, wq, wk, wv, wo)

    tokens, whole = P(("dp", "sp"), None), P(None, None)
    return jax.shard_map(
        step,
        mesh=mesh,
        in_specs=(tokens, P(None), whole, whole, whole, whole),
        out_specs=tokens,
        check_vma=False,
    )
```

```python
import functools
import math

import jax
import jax.numpy as jnp
from jax import lax
from jax.experimental import pallas as pl
from jax.experimental.pallas import tpu as pltpu
from jax.sharding import PartitionSpec as P

HEAD = 128
THETA = 10000
GROUP = 12
FLAGS = ()
NEG = -1e30
HIDDEN = 2 * NEG
LOG2E = 1.4426950408889634
WIDE = 4
STRIP = 512
MESH = pl.DeviceIdType.MESH
VMEM_LIMIT = 67043328


def _dot(a, b):
    return jnp.dot(a, b, preferred_element_type=jnp.float32)


def _kernel(side, groups, x_ref, gain_ref, cos_ref, sin_ref, wq_ref, wk_ref, wv_ref, wo_ref, y_ref,
            xbuf, abuf, wbuf, kv, qt, seen, mix, top, acc, raw,
            wsem, xsem, xsend, xrecv, p1send, p1recv, p2send, p2recv, ssend, srecv, ysem, ysend, yrecv):
    own, depth = x_ref.shape
    tiles = depth // HEAD
    half = wq_ref.shape[1] // 2
    heads = half // HEAD
    kvh = heads // GROUP
    step = WIDE * HEAD
    steps = half // step
    dp, sp = lax.axis_index("dp"), lax.axis_index("sp")
    c = lax.rem(dp, 2)
    other = 1 - c
    partner = {"dp": dp + 1 - 2 * c}
    px, py = lax.div(sp, side), lax.rem(sp, side)

    def device(x, y):
        return {"sp": lax.rem(x + side, side) * side + lax.rem(y + side, side)}

    first = (py, px)
    second = (px, py)
    hop1 = ((device(px, py + 1), device(px, py - 1)), (device(px + 1, py), device(px - 1, py)))
    hop2 = (hop1[1], hop1[0])
    at = lambda p, d: lax.rem(p + d + side, side)

    def tile(ref, n, g, e):
        if 'noload' in FLAGS: return type('N', (), {'start': lambda s: None, 'wait': lambda s: None})()
        src = ref.at[:, pl.ds(pl.multiple_of(n * HEAD, HEAD), HEAD)]
        return pltpu.make_async_copy(src, wbuf.at[g, e], wsem.at[g, e])

    def kv_group():
        return [tile(wk_ref if e < kvh else wv_ref, c * kvh + e % kvh, 0, e) for e in range(WIDE)]

    def q_group(i):
        return [tile(wq_ref, c * heads + i * WIDE + e, lax.rem(i + 1, groups), e) for e in range(WIDE)]

    def o_group(i):
        return [tile(wo_ref, c * heads + i * WIDE + e, lax.rem(i + 1 + steps, groups), e) for e in range(WIDE)]

    def start(copies):
        for copy in copies:
            copy.start()

    def wait(copies):
        for copy in copies:
            copy.wait()

    load_x = pltpu.make_async_copy(x_ref, xbuf.at[c], xsem)
    load_x.start()
    start(kv_group())

    barrier = pltpu.get_barrier_semaphore()
    peers = [partner, *hop1[0], *hop1[1]]
    for peer in peers:
        pl.semaphore_signal(barrier, inc=1, device_id=peer, device_id_type=MESH)
    pl.semaphore_wait(barrier, len(peers))

    def remote(src, dst, send, recv, peer):
        return pltpu.make_async_remote_copy(src_ref=src, dst_ref=dst, send_sem=send, recv_sem=recv, device_id=peer, device_id_type=MESH)

    send_x = remote(x_ref, xbuf.at[c], xsend, xrecv, partner)
    send_x.start()
    for i in range(groups - 1):
        start(q_group(i))

    rows = 16

    def norm(s):
        def body(r, _):
            here = pl.ds(pl.multiple_of(r * rows, rows), rows)
            total = jnp.zeros((rows, HEAD), jnp.float32)
            for t in range(tiles):
                wide = xbuf[s, here, t * HEAD : (t + 1) * HEAD].astype(jnp.float32)
                total += wide * wide
            scale = lax.rsqrt(jnp.sum(total, -1, keepdims=True) / depth + 1e-6)
            place = pl.ds(pl.multiple_of(s * own + r * rows, rows), rows)
            for t in range(tiles):
                cut = slice(t * HEAD, (t + 1) * HEAD)
                wide = xbuf[s, here, cut].astype(jnp.float32)
                abuf[t, place, :] = (wide * scale * gain_ref[t : t + 1, :].astype(jnp.float32)).astype(jnp.bfloat16)

        lax.fori_loop(0, own // rows, body, None)

    def project(g, here=slice(None)):
        lhs = jnp.concatenate([abuf[t, here, :] for t in range(tiles)], axis=1)
        rhs = jnp.concatenate([wbuf[g, e] for e in range(WIDE)], axis=1)
        return _dot(lhs, rhs).astype(jnp.bfloat16)

    def split(t):
        return [(s, e, t[s * own : (s + 1) * own, e * HEAD : (e + 1) * HEAD]) for s in range(2) for e in range(WIDE)]

    def turned(t):
        t = t.astype(jnp.float32)
        return (t * cos_ref[...] + pltpu.roll(t, HEAD // 2, 1) * sin_ref[...]).astype(jnp.bfloat16)

    def rows_of(s):
        return pl.ds(pl.multiple_of(s * own, own), own)

    def project_rows(i, s):
        raw[rows_of(s), :] = project(i, rows_of(s))

    load_x.wait()
    norm(c)
    wait(kv_group())
    project_rows(0, c)
    send_x.wait_recv()
    norm(other)
    project_rows(0, other)
    for s, e, t in split(raw[...]):
        if e < kvh:
            kv[s, second[s], first[s], e, 0] = turned(t)
        else:
            kv[s, second[s], first[s], e - kvh, 1] = t.T

    def piece(s, g, f, h=None):
        ref = kv.at[s, at(second[s], g), at(first[s], f)]
        return ref if h is None else ref.at[h]

    class Nop:
        def start(self): pass
        wait = wait_send = wait_recv = start
    def send(stage, s, n, peer, ref):
        if 'nocomm' in FLAGS: return Nop()
        sends, recvs = (p1send, p1recv) if stage == 1 else (p2send, p2recv)
        return remote(ref, ref, sends.at[(s, *n)], recvs.at[(s, *n)], peer)

    def hop1_copy(s, n):
        if n < 2:
            return send(1, s, (n,), hop1[s][n], piece(s, 0, 0))
        return send(1, s, (n,), hop1[s][n - 2], piece(s, 0, -1 if n == 2 else 1, n - 2))

    def hop1_arrival(s, n):
        ref = piece(s, 0, -1 if n == 0 else 1) if n < 2 else piece(s, 0, 2, n - 2)
        return send(1, s, (n,), hop1[s][n % 2], ref)

    order = (0, -1, 1, 2)

    def hop2_copy(s, n, o):
        if n < 2:
            return send(2, s, (n, o), hop2[s][n], piece(s, 0, order[o]))
        return send(2, s, (n, o), hop2[s][n - 2], piece(s, -1 if n == 2 else 1, order[o], n - 2))

    def hop2_arrival(s, n, o):
        ref = piece(s, -1 if n == 0 else 1, order[o]) if n < 2 else piece(s, 2, order[o], n - 2)
        return send(2, s, (n, o), hop2[s][n % 2], ref)

    both = (0, 1)
    for s in both:
        for n in (0, 1):
            hop1_copy(s, n).start()
    for s in both:
        for n in (0, 1):
            hop2_copy(s, n, 0).start()

    def comm1():
        for s in both:
            for n in (0, 1):
                hop1_arrival(s, n).wait_recv()
                hop1_copy(s, n + 2).start()
        for s in both:
            for o in (1, 2):
                for n in (0, 1):
                    hop2_copy(s, n, o).start()

    def comm2():
        for s in both:
            for n in (2, 3):
                hop1_arrival(s, n).wait_recv()
            for n in (0, 1):
                hop2_copy(s, n, 3).start()
        forward(0)

    def forward(o):
        for s in both:
            for n in (0, 1):
                hop2_arrival(s, n, o).wait_recv()
                hop2_copy(s, n + 2, o).start()

    start(q_group(groups - 1))

    def turn(t, i):
        for s, e, part in split(t):
            qt[s, i * WIDE + e] = turned(part).T

    def q_step(i, _):
        wait(q_group(i))
        before = raw[...]
        now = project(lax.rem(i + 1, groups))
        turn(before, lax.max(i - 1, 0))
        raw[...] = now
        start(o_group(i))

        @pl.when(i == 2)
        def _():
            comm1()

    lax.fori_loop(0, steps, q_step, None)
    comm2()
    turn(raw[...], steps - 1)

    e = HEAD**-0.5 * LOG2E
    cols = GROUP * own
    begin = sp * own
    for s in both:
        for h in range(kvh):
            top[s * kvh + h] = jnp.full((1, cols), NEG, jnp.float32)
            mix[s * kvh + h] = jnp.zeros((HEAD + 8, cols), jnp.float32)

    def unit(s, g, masked):
        keys = side * own
        row = lax.broadcasted_iota(jnp.int32, (keys, STRIP), 0)
        query = lax.rem(lax.broadcasted_iota(jnp.int32, (keys, STRIP), 1), own)
        if masked:
            if s == 0:
                ok = query - row >= g * keys - begin
            else:
                ok = query - (lax.div(row, own) * (side * own) + lax.rem(row, own)) >= g * own - begin
        ones = jnp.ones((8, keys), jnp.bfloat16)
        pieces = [(h, a) for h in range(kvh) for a in range(0, cols, STRIP)]
        per = STRIP // own
        scores = []
        for h, a in pieces:
            k = jnp.concatenate([kv[s, g, f, h, 0] for f in range(side)], axis=0)
            q = jnp.concatenate([qt[s, h * GROUP + a // own + n] for n in range(per)], axis=1)
            scores.append(_dot(k, q))
        weights, keeps = [], []
        for (h, a), sc in zip(pieces, scores):
            if masked:
                sc = jnp.where(ok, sc, HIDDEN)
            old = top[s * kvh + h, :, a : a + STRIP]
            new = jnp.maximum(old, sc.max(axis=0, keepdims=True))
            top[s * kvh + h, :, a : a + STRIP] = new
            weights.append(jnp.exp2((sc - new) * e).astype(jnp.bfloat16))
            keeps.append(jnp.exp2((old - new) * e))
        for (h, a), p, keep in zip(pieces, weights, keeps):
            values = jnp.concatenate([jnp.concatenate([kv[s, g, f, h, 1] for f in range(side)], axis=1), ones], axis=0)
            mix[s * kvh + h, :, a : a + STRIP] = mix[s * kvh + h, :, a : a + STRIP] * keep + _dot(values, p)

    def attend(t, _):
        @pl.when(t == 1)
        def _():
            forward(1)
            forward(2)
            forward(3)

        @pl.when(t == 3)
        def _():
            for s in both:
                for n in (2, 3):
                    for o in range(side):
                        hop2_arrival(s, n, o).wait_recv()

        d = (lax.rem(t + 1, 3) + 1) * lax.div(t + 3, 4)
        for s in (() if 'noattn' in FLAGS else both):
            g = at(second[s], d)
            if s == 0:
                some, whole = g <= px, g < px
            else:
                some = g * own <= begin
                whole = (side - 1) * side * own + g * own < begin

            @pl.when(whole)
            def _():
                unit(s, g, False)

            @pl.when(some & jnp.logical_not(whole))
            def _():
                unit(s, g, True)

    lax.fori_loop(0, side, attend, None)

    def seen_part(which, s, h):
        return seen.at[which, pl.ds(h * GROUP, GROUP), pl.ds(s * own, own)]

    def seen_copy(which, s, h):
        return remote(seen_part(which, s, h), seen_part(which, s, h), ssend.at[s, h], srecv.at[s, h], partner)

    for s in both:
        for h in range(kvh):
            over = 1 / mix[s * kvh + h, HEAD : HEAD + 1, :]
            for n in range(GROUP):
                cut = slice(n * own, (n + 1) * own)
                out = mix[s * kvh + h, :HEAD, cut] * over[:, cut]
                seen[c, h * GROUP + n, s * own : (s + 1) * own] = out.T.astype(jnp.bfloat16)
            seen_copy(c, s, h).start()

    def o_part(which, i):
        g = lax.rem(i + 1 + steps, groups)
        there = pl.ds(pl.multiple_of(which * half, half), half)
        lhs = jnp.concatenate([seen[which, t] for t in range(heads)], axis=1)
        rhs = jnp.concatenate([wbuf[g, e, there, :] for e in range(WIDE)], axis=1)
        return _dot(lhs, rhs)

    def o_step1(j, _):
        for i in (2 * j, 2 * j + 1):
            wait(o_group(i))
        for i in (2 * j, 2 * j + 1):
            acc[i] = o_part(c, i)

    lax.fori_loop(0, steps // 2, o_step1, None)
    for s in both:
        for h in range(kvh):
            seen_copy(other, s, h).wait_recv()

    def y_copies(i):
        cut = pl.ds(pl.multiple_of(c * half + i * step, step), step)
        coming = pl.ds(pl.multiple_of(other * half + i * step, step), step)
        return (pltpu.make_async_copy(xbuf.at[c, :, cut], y_ref.at[:, cut], ysem.at[i]),
                lambda: remote(xbuf.at[other, :, cut], y_ref.at[:, cut], ysend.at[i], yrecv.at[i], partner),
                lambda: remote(xbuf.at[other, :, cut], y_ref.at[:, coming], ysend.at[i], yrecv.at[i], partner))

    def o_step2(i, _):
        cut = pl.ds(pl.multiple_of(c * half + i * step, step), step)
        y = (acc[i] + o_part(other, i)) + xbuf[:, :, cut].reshape(2 * own, step).astype(jnp.float32)
        xbuf[:, :, cut] = y.astype(jnp.bfloat16).reshape(2, own, step)
        mine, theirs, _ = y_copies(i)
        mine.start()
        theirs().start()

    lax.fori_loop(0, steps, o_step2, None)

    for i in range(steps):
        mine, theirs, coming = y_copies(i)
        mine.wait()
        theirs().wait_send()
        coming().wait_recv()
    send_x.wait_send()
    for s in both:
        for h in range(kvh):
            seen_copy(c, s, h).wait_send()
        for n in range(4):
            hop1_copy(s, n).wait_send()
            for o in range(side):
                hop2_copy(s, n, o).wait_send()


def solution(mesh):
    side = math.isqrt(mesh.shape["sp"])

    def step(x, gain, wq, wk, wv, wo):
        own, depth = x.shape
        half = wq.shape[1] // 2
        heads, kvh = half // HEAD, half // HEAD // GROUP
        steps = half // (WIDE * HEAD)
        groups = steps
        cols = GROUP * own
        place = (lax.axis_index("sp") * own + jnp.arange(own)).astype(jnp.float32)
        lane = jnp.arange(HEAD)
        angle = place[:, None] * THETA ** (-(lane % (HEAD // 2)).astype(jnp.float32) / (HEAD // 2))
        cos, sin = jnp.cos(angle), jnp.where(lane < HEAD // 2, -1.0, 1.0) * jnp.sin(angle)
        bf, f32, dma = jnp.bfloat16, jnp.float32, pltpu.SemaphoreType.DMA
        vmem, hbm = pl.BlockSpec(memory_space=pltpu.VMEM), pl.BlockSpec(memory_space=pl.ANY)
        return pl.pallas_call(
            functools.partial(_kernel, side, groups),
            out_shape=jax.ShapeDtypeStruct((own, depth), bf),
            in_specs=[hbm, vmem, vmem, vmem, hbm, hbm, hbm, hbm],
            out_specs=hbm,
            scratch_shapes=[
                pltpu.VMEM((2, own, depth), bf),
                pltpu.VMEM((depth // HEAD, 2 * own, HEAD), bf),
                pltpu.VMEM((groups, WIDE, depth, HEAD), bf),
                pltpu.VMEM((2, side, side, kvh, 2, own, HEAD), bf),
                pltpu.VMEM((2, heads, HEAD, own), bf),
                pltpu.VMEM((2, heads, 2 * own, HEAD), bf),
                pltpu.VMEM((2 * kvh, HEAD + 8, cols), f32),
                pltpu.VMEM((2 * kvh, 1, cols), f32),
                pltpu.VMEM((steps, 2 * own, WIDE * HEAD), f32),
                pltpu.VMEM((2 * own, WIDE * HEAD), bf),
                dma((groups, WIDE)), dma, dma, dma,
                dma((2, 4)), dma((2, 4)), dma((2, 4, side)), dma((2, 4, side)),
                dma((2, kvh)), dma((2, kvh)),
                dma((steps,)), dma((steps,)), dma((steps,)),
            ],
            compiler_params=pltpu.CompilerParams(collective_id=0, has_side_effects=True, vmem_limit_bytes=VMEM_LIMIT),
        )(x, gain.reshape(-1, HEAD), cos, sin, wq, wk, wv, wo)

    tokens, whole = P(("dp", "sp"), None), P(None, None)
    return jax.shard_map(
        step,
        mesh=mesh,
        in_specs=(tokens, P(None), whole, whole, whole, whole),
        out_specs=tokens,
        check_vma=False,
    )
```

```python
import functools
import math

import jax
import jax.numpy as jnp
import numpy as np
from jax import lax
from jax.experimental import pallas as pl
from jax.experimental.pallas import tpu as pltpu
from jax.sharding import PartitionSpec as P

HEAD = 128
THETA = 10000
GROUP = 12
FLAGS = ()
NEG = -1e30
HIDDEN = 2 * NEG
LOG2E = 1.4426950408889634
WIDE = 4
STRIP = 512
MESH = pl.DeviceIdType.MESH
VMEM_LIMIT = 67043328


def _dot(a, b):
    return jnp.dot(a, b, preferred_element_type=jnp.float32)


def _kernel(side, groups, x_ref, gain_ref, table_ref, wq_ref, wk_ref, wv_ref, wo_ref, y_ref,
            xbuf, abuf, wbuf, kv, qt, seen, mix, top, acc, raw, cos_ref, sin_ref, tsem,
            wsem, xsem, xsend, xrecv, p1send, p1recv, p2send, p2recv, ssend, srecv, ysem, ysend, yrecv):
    own, depth = x_ref.shape
    tiles = depth // HEAD
    half = wq_ref.shape[1] // 2
    heads = half // HEAD
    kvh = heads // GROUP
    step = WIDE * HEAD
    steps = half // step
    dp, sp = lax.axis_index("dp"), lax.axis_index("sp")
    c = lax.rem(dp, 2)
    other = 1 - c
    partner = {"dp": dp + 1 - 2 * c}
    px, py = lax.div(sp, side), lax.rem(sp, side)

    def device(x, y):
        return {"sp": lax.rem(x + side, side) * side + lax.rem(y + side, side)}

    first = (py, px)
    second = (px, py)
    hop1 = ((device(px, py + 1), device(px, py - 1)), (device(px + 1, py), device(px - 1, py)))
    hop2 = (hop1[1], hop1[0])
    at = lambda p, d: lax.rem(p + d + side, side)

    def tile(ref, n, g, e):
        if 'noload' in FLAGS: return type('N', (), {'start': lambda s: None, 'wait': lambda s: None})()
        src = ref.at[:, pl.ds(pl.multiple_of(n * HEAD, HEAD), HEAD)]
        return pltpu.make_async_copy(src, wbuf.at[g, e], wsem.at[g, e])

    def kv_group():
        return [tile(wk_ref if e < kvh else wv_ref, c * kvh + e % kvh, 0, e) for e in range(WIDE)]

    def q_group(i):
        return [tile(wq_ref, c * heads + i * WIDE + e, lax.rem(i + 1, groups), e) for e in range(WIDE)]

    def o_group(i):
        return [tile(wo_ref, c * heads + i * WIDE + e, lax.rem(i + 1 + steps, groups), e) for e in range(WIDE)]

    def start(copies):
        for copy in copies:
            copy.start()

    def wait(copies):
        for copy in copies:
            copy.wait()

    load_x = pltpu.make_async_copy(x_ref, xbuf.at[c], xsem)
    load_x.start()
    load_table = pltpu.make_async_copy(table_ref.at[pl.ds(pl.multiple_of(sp * own, own), own)], cos_ref, tsem)
    load_table.start()
    start(kv_group())

    barrier = pltpu.get_barrier_semaphore()
    peers = [partner, *hop1[0], *hop1[1]]
    for peer in peers:
        pl.semaphore_signal(barrier, inc=1, device_id=peer, device_id_type=MESH)
    pl.semaphore_wait(barrier, len(peers))

    def remote(src, dst, send, recv, peer):
        return pltpu.make_async_remote_copy(src_ref=src, dst_ref=dst, send_sem=send, recv_sem=recv, device_id=peer, device_id_type=MESH)

    send_x = remote(x_ref, xbuf.at[c], xsend, xrecv, partner)
    send_x.start()
    for i in range(groups - 1):
        start(q_group(i))

    rows = 16

    def norm(s):
        def body(r, _):
            here = pl.ds(pl.multiple_of(r * rows, rows), rows)
            total = jnp.zeros((rows, HEAD), jnp.float32)
            for t in range(tiles):
                wide = xbuf[s, here, t * HEAD : (t + 1) * HEAD].astype(jnp.float32)
                total += wide * wide
            scale = lax.rsqrt(jnp.sum(total, -1, keepdims=True) / depth + 1e-6)
            place = pl.ds(pl.multiple_of(s * own + r * rows, rows), rows)
            for t in range(tiles):
                cut = slice(t * HEAD, (t + 1) * HEAD)
                wide = xbuf[s, here, cut].astype(jnp.float32)
                abuf[t, place, :] = (wide * scale * gain_ref[t : t + 1, :].astype(jnp.float32)).astype(jnp.bfloat16)

        lax.fori_loop(0, own // rows, body, None)

    def project(g, here=slice(None)):
        lhs = jnp.concatenate([abuf[t, here, :] for t in range(tiles)], axis=1)
        rhs = jnp.concatenate([wbuf[g, e] for e in range(WIDE)], axis=1)
        return _dot(lhs, rhs).astype(jnp.bfloat16)

    def split(t):
        return [(s, e, t[s * own : (s + 1) * own, e * HEAD : (e + 1) * HEAD]) for s in range(2) for e in range(WIDE)]

    def turned(t):
        t = t.astype(jnp.float32)
        return (t * cos_ref[...] + pltpu.roll(t, HEAD // 2, 1) * sin_ref[...]).astype(jnp.bfloat16)

    def rows_of(s):
        return pl.ds(pl.multiple_of(s * own, own), own)

    def project_rows(i, s):
        raw[rows_of(s), :] = project(i, rows_of(s))

    load_x.wait()
    norm(c)
    load_table.wait()
    table = cos_ref[...]
    swapped, early = pltpu.roll(table, HEAD // 2, 1), lax.broadcasted_iota(jnp.int32, table.shape, 1) < HEAD // 2
    cos_ref[...] = jnp.where(early, table, swapped)
    sin_ref[...] = jnp.where(early, -swapped, table)
    wait(kv_group())
    project_rows(0, c)
    send_x.wait_recv()
    norm(other)
    project_rows(0, other)
    for s, e, t in split(raw[...]):
        if e < kvh:
            kv[s, second[s], first[s], e, 0] = turned(t)
        else:
            kv[s, second[s], first[s], e - kvh, 1] = t.T

    def piece(s, g, f, h=None):
        ref = kv.at[s, at(second[s], g), at(first[s], f)]
        return ref if h is None else ref.at[h]

    class Nop:
        def start(self): pass
        wait = wait_send = wait_recv = start
    def send(stage, s, n, peer, ref):
        if 'nocomm' in FLAGS: return Nop()
        sends, recvs = (p1send, p1recv) if stage == 1 else (p2send, p2recv)
        return remote(ref, ref, sends.at[(s, *n)], recvs.at[(s, *n)], peer)

    def hop1_copy(s, n):
        if n < 2:
            return send(1, s, (n,), hop1[s][n], piece(s, 0, 0))
        return send(1, s, (n,), hop1[s][n - 2], piece(s, 0, -1 if n == 2 else 1, n - 2))

    def hop1_arrival(s, n):
        ref = piece(s, 0, -1 if n == 0 else 1) if n < 2 else piece(s, 0, 2, n - 2)
        return send(1, s, (n,), hop1[s][n % 2], ref)

    order = (0, -1, 1, 2)

    def hop2_copy(s, n, o):
        if n < 2:
            return send(2, s, (n, o), hop2[s][n], piece(s, 0, order[o]))
        return send(2, s, (n, o), hop2[s][n - 2], piece(s, -1 if n == 2 else 1, order[o], n - 2))

    def hop2_arrival(s, n, o):
        ref = piece(s, -1 if n == 0 else 1, order[o]) if n < 2 else piece(s, 2, order[o], n - 2)
        return send(2, s, (n, o), hop2[s][n % 2], ref)

    both = (0, 1)
    for s in both:
        for n in (0, 1):
            hop1_copy(s, n).start()
    for s in both:
        for n in (0, 1):
            hop2_copy(s, n, 0).start()

    def comm1():
        for s in both:
            for n in (0, 1):
                hop1_arrival(s, n).wait_recv()
                hop1_copy(s, n + 2).start()
        for s in both:
            for o in (1, 2):
                for n in (0, 1):
                    hop2_copy(s, n, o).start()

    def comm2():
        for s in both:
            for n in (2, 3):
                hop1_arrival(s, n).wait_recv()
            for n in (0, 1):
                hop2_copy(s, n, 3).start()
        forward(0)

    def forward(o):
        for s in both:
            for n in (0, 1):
                hop2_arrival(s, n, o).wait_recv()
                hop2_copy(s, n + 2, o).start()

    start(q_group(groups - 1))

    def turn(t, i):
        for s, e, part in split(t):
            qt[s, i * WIDE + e] = turned(part).T

    def q_step(i, _):
        wait(q_group(i))
        before = raw[...]
        now = project(lax.rem(i + 1, groups))
        turn(before, lax.max(i - 1, 0))
        raw[...] = now
        start(o_group(i))

        @pl.when(i == 2)
        def _():
            comm1()

    lax.fori_loop(0, steps, q_step, None)
    comm2()
    turn(raw[...], steps - 1)

    e = HEAD**-0.5 * LOG2E
    cols = GROUP * own
    begin = sp * own
    for s in both:
        for h in range(kvh):
            top[s * kvh + h] = jnp.full((1, cols), NEG, jnp.float32)
            mix[s * kvh + h] = jnp.zeros((HEAD + 8, cols), jnp.float32)

    def unit(s, g, masked):
        keys = side * own
        row = lax.broadcasted_iota(jnp.int32, (keys, STRIP), 0)
        query = lax.rem(lax.broadcasted_iota(jnp.int32, (keys, STRIP), 1), own)
        if masked:
            if s == 0:
                ok = query - row >= g * keys - begin
            else:
                ok = query - (lax.div(row, own) * (side * own) + lax.rem(row, own)) >= g * own - begin
        ones = jnp.ones((8, keys), jnp.bfloat16)
        pieces = [(h, a) for h in range(kvh) for a in range(0, cols, STRIP)]
        per = STRIP // own
        scores = []
        for h, a in pieces:
            k = jnp.concatenate([kv[s, g, f, h, 0] for f in range(side)], axis=0)
            q = jnp.concatenate([qt[s, h * GROUP + a // own + n] for n in range(per)], axis=1)
            scores.append(_dot(k, q))
        weights, keeps = [], []
        for (h, a), sc in zip(pieces, scores):
            if masked:
                sc = jnp.where(ok, sc, HIDDEN)
            old = top[s * kvh + h, :, a : a + STRIP]
            new = jnp.maximum(old, sc.max(axis=0, keepdims=True))
            top[s * kvh + h, :, a : a + STRIP] = new
            weights.append(jnp.exp2((sc - new) * e).astype(jnp.bfloat16))
            keeps.append(jnp.exp2((old - new) * e))
        for (h, a), p, keep in zip(pieces, weights, keeps):
            values = jnp.concatenate([jnp.concatenate([kv[s, g, f, h, 1] for f in range(side)], axis=1), ones], axis=0)
            mix[s * kvh + h, :, a : a + STRIP] = mix[s * kvh + h, :, a : a + STRIP] * keep + _dot(values, p)

    def attend(t, _):
        @pl.when(t == 1)
        def _():
            forward(1)
            forward(2)
            forward(3)

        @pl.when(t == 3)
        def _():
            for s in both:
                for n in (2, 3):
                    for o in range(side):
                        hop2_arrival(s, n, o).wait_recv()

        d = (lax.rem(t + 1, 3) + 1) * lax.div(t + 3, 4)
        for s in (() if 'noattn' in FLAGS else both):
            g = at(second[s], d)
            if s == 0:
                some, whole = g <= px, g < px
            else:
                some = g * own <= begin
                whole = (side - 1) * side * own + g * own < begin

            @pl.when(whole)
            def _():
                unit(s, g, False)

            @pl.when(some & jnp.logical_not(whole))
            def _():
                unit(s, g, True)

    lax.fori_loop(0, side, attend, None)

    def seen_part(which, s, h):
        return seen.at[which, pl.ds(h * GROUP, GROUP), pl.ds(s * own, own)]

    def seen_copy(which, s, h):
        return remote(seen_part(which, s, h), seen_part(which, s, h), ssend.at[s, h], srecv.at[s, h], partner)

    for s in both:
        for h in range(kvh):
            over = 1 / mix[s * kvh + h, HEAD : HEAD + 1, :]
            for n in range(GROUP):
                cut = slice(n * own, (n + 1) * own)
                out = mix[s * kvh + h, :HEAD, cut] * over[:, cut]
                seen[c, h * GROUP + n, s * own : (s + 1) * own] = out.T.astype(jnp.bfloat16)
            seen_copy(c, s, h).start()

    def o_part(which, i):
        g = lax.rem(i + 1 + steps, groups)
        there = pl.ds(pl.multiple_of(which * half, half), half)
        lhs = jnp.concatenate([seen[which, t] for t in range(heads)], axis=1)
        rhs = jnp.concatenate([wbuf[g, e, there, :] for e in range(WIDE)], axis=1)
        return _dot(lhs, rhs)

    def o_step1(j, _):
        for i in (2 * j, 2 * j + 1):
            wait(o_group(i))
        for i in (2 * j, 2 * j + 1):
            acc[i] = o_part(c, i)

    lax.fori_loop(0, steps // 2, o_step1, None)
    for s in both:
        for h in range(kvh):
            seen_copy(other, s, h).wait_recv()

    def y_copies(i):
        cut = pl.ds(pl.multiple_of(c * half + i * step, step), step)
        coming = pl.ds(pl.multiple_of(other * half + i * step, step), step)
        return (pltpu.make_async_copy(xbuf.at[c, :, cut], y_ref.at[:, cut], ysem.at[i]),
                lambda: remote(xbuf.at[other, :, cut], y_ref.at[:, cut], ysend.at[i], yrecv.at[i], partner),
                lambda: remote(xbuf.at[other, :, cut], y_ref.at[:, coming], ysend.at[i], yrecv.at[i], partner))

    def o_step2(i, _):
        cut = pl.ds(pl.multiple_of(c * half + i * step, step), step)
        y = (acc[i] + o_part(other, i)) + xbuf[:, :, cut].reshape(2 * own, step).astype(jnp.float32)
        xbuf[:, :, cut] = y.astype(jnp.bfloat16).reshape(2, own, step)
        mine, theirs, _ = y_copies(i)
        mine.start()
        theirs().start()

    lax.fori_loop(0, steps, o_step2, None)

    for i in range(steps):
        mine, theirs, coming = y_copies(i)
        mine.wait()
        theirs().wait_send()
        coming().wait_recv()
    send_x.wait_send()
    for s in both:
        for h in range(kvh):
            seen_copy(c, s, h).wait_send()
        for n in range(4):
            hop1_copy(s, n).wait_send()
            for o in range(side):
                hop2_copy(s, n, o).wait_send()


def solution(mesh):
    side = math.isqrt(mesh.shape["sp"])

    def step(x, gain, wq, wk, wv, wo):
        own, depth = x.shape
        half = wq.shape[1] // 2
        heads, kvh = half // HEAD, half // HEAD // GROUP
        steps = half // (WIDE * HEAD)
        groups = steps
        cols = GROUP * own
        angle = np.arange(mesh.shape["sp"] * own, dtype=np.float32)[:, None] * np.float32(THETA) ** (
            -np.arange(HEAD // 2, dtype=np.float32) / np.float32(HEAD // 2))
        table = jnp.asarray(np.concatenate([np.cos(angle), np.sin(angle)], -1).astype(np.float32))
        bf, f32, dma = jnp.bfloat16, jnp.float32, pltpu.SemaphoreType.DMA
        vmem, hbm = pl.BlockSpec(memory_space=pltpu.VMEM), pl.BlockSpec(memory_space=pl.ANY)
        return pl.pallas_call(
            functools.partial(_kernel, side, groups),
            out_shape=jax.ShapeDtypeStruct((own, depth), bf),
            in_specs=[hbm, vmem, hbm, hbm, hbm, hbm, hbm],
            out_specs=hbm,
            scratch_shapes=[
                pltpu.VMEM((2, own, depth), bf),
                pltpu.VMEM((depth // HEAD, 2 * own, HEAD), bf),
                pltpu.VMEM((groups, WIDE, depth, HEAD), bf),
                pltpu.VMEM((2, side, side, kvh, 2, own, HEAD), bf),
                pltpu.VMEM((2, heads, HEAD, own), bf),
                pltpu.VMEM((2, heads, 2 * own, HEAD), bf),
                pltpu.VMEM((2 * kvh, HEAD + 8, cols), f32),
                pltpu.VMEM((2 * kvh, 1, cols), f32),
                pltpu.VMEM((steps, 2 * own, WIDE * HEAD), f32),
                pltpu.VMEM((2 * own, WIDE * HEAD), bf),
                pltpu.VMEM((own, HEAD), f32),
                pltpu.VMEM((own, HEAD), f32),
                dma,
                dma((groups, WIDE)), dma, dma, dma,
                dma((2, 4)), dma((2, 4)), dma((2, 4, side)), dma((2, 4, side)),
                dma((2, kvh)), dma((2, kvh)),
                dma((steps,)), dma((steps,)), dma((steps,)),
            ],
            compiler_params=pltpu.CompilerParams(collective_id=0, has_side_effects=True, vmem_limit_bytes=VMEM_LIMIT),
        )(x, gain.reshape(-1, HEAD), table, wq, wk, wv, wo)

    tokens, whole = P(("dp", "sp"), None), P(None, None)
    return jax.shard_map(
        step,
        mesh=mesh,
        in_specs=(tokens, P(None), whole, whole, whole, whole),
        out_specs=tokens,
        check_vma=False,
    )
```
